32 devices in a mesh: groups: 1, ctx: 32 (over z, y, x, core).
Axes of the slice: x: 2, y: 2, z: 4, core: 2. Of those that a mesh axis runs over, the one named last changes fastest.
Arguments:
- prefill_query: bfloat16 [1024, 32, 576], P('groups', 'ctx'), may hold values from -1000 to 1000
- prefill_latent: bfloat16 [1024, 576], P(('groups', 'ctx')), may hold values from -6 to 6
- decode_query: bfloat16 [2, 32, 576], P('groups'), may hold values from -1000 to 1000
- cache: bfloat16 [2, 16384, 576], P('groups', 'ctx'), may hold values from -6 to 6
- lengths: int32 [2], P('groups'), may hold values from 2049 to 16384
- page_table: int32 [64, 2], P('groups'), may hold values from 0 to 31, as said below
Outputs:
- prefill_out: bfloat16 [1024, 32, 512], P('groups', 'ctx')
- decode_out: bfloat16 [2, 32, 512], P('groups', 'ctx')
The draws below stay inside these ranges and needn't reach their ends.
Inputs may be any that keep to these rules, and one draw needn't show every extreme that they name: `page_table`: row p names the device (column 0, below 32) and the pool slot (column 1, below 16) that take latent page p; no two rows name the same pair.
All inputs are finite; a program needn't handle non-finite values.
Results may differ from the reference program's by a relative error of at most 0.0049.
Values may be sent and summed in bfloat16 or wider, within the bound.
A program may use at most 64 MiB of HBM per device.

```python
import jax
import jax.numpy as jnp
from jax import lax

D_LAT = 512
D_ROPE = 64
PAGE = 16
POOL = 16
SPAN = 1024
REQ = 2
HEADS = 32
CTXLEN = 16384
NPAGES = 64
N_CTX = 32


SCALE = 192.0 ** (-0.5)


def cache_block(key, request, block):
    sub_key = jax.random.fold_in(jax.random.fold_in(jax.random.fold_in(key, 501), request), block)
    raw = jax.random.normal(sub_key, (64, D_LAT + D_ROPE), jnp.float32)
    return jnp.clip(raw, -6.0, 6.0).astype(jnp.bfloat16).astype(jnp.float32)


def cache_row(key, request, position):
    return cache_block(key, request, position // 64)[position % 64]


def latent_matrix(key):
    raw = jax.random.normal(jax.random.fold_in(key, 502), (SPAN, D_LAT + D_ROPE), jnp.float32)
    return jnp.clip(raw, -6.0, 6.0).astype(jnp.bfloat16).astype(jnp.float32)


def aligned(first, second, strength):
    self_first = jnp.sum(first * first, axis=-1)
    self_second = jnp.sum(second * second, axis=-1)
    cross = jnp.sum(first * second, axis=-1)
    coefficient = (strength * (self_first - cross) - 2.0 / SCALE) / (self_second - cross)
    return strength[..., None] * first + coefficient[..., None] * second


def strength_table():
    return jnp.array([3.0, 5.0, 8.0], jnp.float32) * (576.0 / (D_LAT + D_ROPE))


def prefill_built(key):
    latent = latent_matrix(key)
    picked = HEADS // 16
    row_index = jnp.arange(SPAN)[:, None]
    head_index = jnp.arange(picked)[None, :]
    other = jax.random.randint(jax.random.fold_in(key, 512), (SPAN, picked), 0, SPAN) % jnp.maximum(row_index, 1)
    strength = strength_table()[(head_index + row_index) % 3]
    first = latent[jnp.broadcast_to(row_index, (SPAN, picked))]
    second = latent[other]
    built = aligned(first, second, strength)
    chosen = jnp.broadcast_to(row_index % 64 == 63, (SPAN, picked))
    return (built, chosen)


def decode_built(key):
    picked = HEADS // 16
    reach = CTXLEN // 8
    first_pos = jax.random.randint(jax.random.fold_in(key, 522), (REQ, picked), 0, reach)
    step_pos = jax.random.randint(jax.random.fold_in(key, 523), (REQ, picked), 1, reach)
    second_pos = (first_pos + step_pos) % reach
    request_index = jnp.broadcast_to(jnp.arange(REQ)[:, None], (REQ, picked))
    head_index = jnp.arange(picked)[None, :]
    row_fetch = jax.vmap(jax.vmap(lambda request, position: cache_row(key, request, position)))
    first = row_fetch(request_index, first_pos)
    second = row_fetch(request_index, second_pos)
    strength = strength_table()[(head_index + request_index) % 3]
    return aligned(first, second, strength)


def draw_cache(key, part):
    blocks = CTXLEN // 64
    full = jax.vmap(lambda request: jax.vmap(lambda block: cache_block(key, request, block))(jnp.arange(blocks)))(jnp.arange(REQ))
    return full.reshape(REQ, CTXLEN, D_LAT + D_ROPE).astype(jnp.bfloat16)


def draw_prefill_latent(key, part):
    return latent_matrix(key).astype(jnp.bfloat16)


def draw_prefill_query(key, part):
    width = D_LAT + D_ROPE
    plain = 2.0 * jnp.clip(jax.random.normal(jax.random.fold_in(key, 513), (SPAN, HEADS, width), jnp.float32), -6.0, 6.0)
    built, chosen = prefill_built(key)
    query = plain.at[:, ::16, :].set(jnp.where(chosen[..., None], built, plain[:, ::16, :]))
    return jnp.clip(query, -1000.0, 1000.0).astype(jnp.bfloat16)


def draw_decode_query(key, part):
    width = D_LAT + D_ROPE
    plain = 2.0 * jnp.clip(jax.random.normal(jax.random.fold_in(key, 524), (REQ, HEADS, width), jnp.float32), -6.0, 6.0)
    query = plain.at[:, ::16, :].set(decode_built(key))
    return jnp.clip(query, -1000.0, 1000.0).astype(jnp.bfloat16)


def draw_page_table(key, part):
    order = jax.random.permutation(jax.random.fold_in(key, 531), N_CTX * POOL)[:NPAGES]
    return jnp.stack([order // POOL, order % POOL], axis=1).astype(jnp.int32)


def setup_inputs(seed: int = 0, part: int = 0) -> dict:
    keys = jax.random.split(jax.random.key(seed), 7)
    own_keys = jax.random.split(jax.random.fold_in(keys[6], part), 7)
    prefill_query = draw_prefill_query(jax.random.fold_in(jax.random.fold_in(keys[6], part), 71), part)
    prefill_latent = draw_prefill_latent(jax.random.fold_in(jax.random.fold_in(keys[6], part), 71), part)
    decode_query = draw_decode_query(jax.random.fold_in(jax.random.fold_in(keys[6], part), 71), part)
    cache = draw_cache(jax.random.fold_in(jax.random.fold_in(keys[6], part), 71), part)
    lengths = jax.random.randint(own_keys[4], (REQ,), CTXLEN // 8 + 1, CTXLEN + 1).astype(jnp.int32)
    page_table = draw_page_table(jax.random.fold_in(jax.random.fold_in(keys[6], part), 71), part)
    return dict(prefill_query=prefill_query, prefill_latent=prefill_latent, decode_query=decode_query, cache=cache, lengths=lengths, page_table=page_table)


SCALE = 192.0 ** -0.5
NEG = -1.0e30


def softmax_values(scores, allowed, values):
    masked = jnp.where(allowed, scores, NEG)
    top_score = jnp.max(masked, axis=-1, keepdims=True)
    weights = jnp.where(allowed, jnp.exp(scores - top_score), 0.0)
    weight_sum = jnp.sum(weights, axis=-1, keepdims=True)
    mixed = jnp.dot(weights.astype(jnp.bfloat16), values, preferred_element_type=jnp.float32)
    return mixed / weight_sum


def reference(prefill_query, prefill_latent, decode_query, cache, lengths, page_table):
    latent_values = prefill_latent[:, :D_LAT]
    causal = jnp.arange(SPAN, dtype=jnp.int32)[:, None] >= jnp.arange(SPAN, dtype=jnp.int32)[None, :]

    def one_head(queries):
        scores = jnp.dot(queries, prefill_latent.T, preferred_element_type=jnp.float32) * SCALE
        return softmax_values(scores, causal, latent_values).astype(jnp.bfloat16)

    per_head = lax.map(one_head, jnp.swapaxes(prefill_query, 0, 1))
    prefill_out = jnp.swapaxes(per_head, 0, 1)

    page_request = (page_table[:, 0] * POOL + page_table[:, 1]) % REQ
    token_request = jnp.repeat(page_request, PAGE)
    positions = jnp.arange(CTXLEN, dtype=jnp.int32)

    def one_request(request):
        queries = decode_query[request]
        rows_cache = cache[request]
        cache_scores = jnp.dot(queries, rows_cache.T, preferred_element_type=jnp.float32) * SCALE
        page_scores = jnp.dot(queries, prefill_latent.T, preferred_element_type=jnp.float32) * SCALE
        scores = jnp.concatenate([cache_scores, page_scores], axis=1)
        allowed = jnp.concatenate([positions < lengths[request], token_request == request])[None, :]
        values = jnp.concatenate([rows_cache[:, :D_LAT], latent_values], axis=0)
        return softmax_values(scores, allowed, values).astype(jnp.bfloat16)

    decode_out = lax.map(one_request, jnp.arange(REQ, dtype=jnp.int32))
    return prefill_out, decode_out
```

```python
import functools

import jax
import jax.numpy as jnp
from jax import lax
from jax.experimental import pallas as pl
from jax.experimental.pallas import tpu as pltpu
from jax.sharding import PartitionSpec as P

D_LAT = 512
PAGE = 16
POOL = 16
REQ = 2

SCALE = 192.0 ** (-0.5)
NEG = -1e30
MSG = D_LAT + 128


def kernel(
    n,
    qt_hbm,
    lat_hbm,
    dq_ref,
    ct_hbm,
    len_ref,
    pt_ref,
    pout_ref,
    dout_ref,
    held,
    qt,
    q,
    ct,
    parts,
    moved,
    local_sem,
    z_sem,
    x_sem,
    y_sem,
    pair_sem,
    dx_sem,
    dy_sem,
    full_sem,
    half_sem,
    dsend_sem,
    drecv_sem,
):
    me = lax.axis_index("ctx")
    line = n // 8
    core = me % 2
    x = (me // 2) % 2
    y = (me // 4) % 2
    z = me // 8
    rows = lat_hbm.shape[0]
    heads = dq_ref.shape[1]
    span = qt.shape[1]
    cache_dev = ct.shape[2]

    def block(step, by, bx, bc):
        return ((((z + step) % line) * 2 + by) * 2 + bx) * 2 + bc

    def device(step, dy, dx, dc):
        return ((((z + line - step) % line) * 2 + dy) * 2 + dx) * 2 + dc

    x_peer = device(0, y, 1 - x, core)
    y_peer = device(0, 1 - y, x, core)
    pair = device(0, y, x, 1 - core)

    own_copy = pltpu.make_async_copy(lat_hbm, held.at[me], local_sem.at[0])
    own_copy.start()
    q_copy = pltpu.make_async_copy(qt_hbm, qt, local_sem.at[1])
    q_copy.start()
    c_copy = pltpu.make_async_copy(ct_hbm, ct, local_sem.at[2])
    c_copy.start()

    barrier = pltpu.get_barrier_semaphore()

    def greet(step, carry):
        pl.semaphore_signal(barrier, inc=1, device_id={"ctx": (me + step) % n})
        return carry

    lax.fori_loop(1, n, greet, 0)

    split = rows // 2 if rows % 32 == 0 else rows

    def move(index, send, recv, target, part=None):
        ref = held.at[index]
        if part == 0:
            ref = held.at[index, pl.ds(0, split)]
        if part == 1:
            ref = held.at[index, pl.ds(split, rows - split)]
        return pltpu.make_async_remote_copy(
            src_ref=ref, dst_ref=ref, send_sem=send, recv_sem=recv, device_id={"ctx": target}
        )

    sends = []

    def go(copy):
        copy.start()
        sends.append(copy)

    def to_pair(step, by, bx):
        index = block(step, by, bx, core)
        spot = (step * 2 + (0 if by is y else 1)) * 2 + (0 if bx is x else 1)
        go(move(index, pair_sem.at[spot], full_sem.at[index], pair))

    def full_wait(index):
        move(index, z_sem.at[0], full_sem.at[index], pair).wait_recv()

    def half_wait(index):
        move(index, z_sem.at[0], half_sem.at[index, 0], pair, 0).wait_recv()
        if split < rows:
            move(index, z_sem.at[0], half_sem.at[index, 1], pair, 1).wait_recv()

    far_x, far_y = 1 - x, 1 - y

    def spread_column(step):
        index = block(step, y, x, core)
        go(move(index, x_sem.at[step], full_sem.at[index], x_peer))
        go(move(index, y_sem.at[step], full_sem.at[index], y_peer))
        to_pair(step, y, x)

    def spread_plane(step):
        index = block(step, y, far_x, core)
        full_wait(index)
        if split < rows:
            go(move(index, dy_sem.at[step], half_sem.at[index, 1], y_peer, 1))
        to_pair(step, y, far_x)
        index = block(step, far_y, x, core)
        full_wait(index)
        go(move(index, dx_sem.at[step], half_sem.at[index, 0], x_peer, 0))
        to_pair(step, far_y, x)

    own_copy.wait()
    pl.semaphore_wait(barrier, n - 1)

    for step in range(line - 1, 0, -1):
        go(move(me, z_sem.at[step], full_sem.at[me], device(step, y, x, core)))
    spread_column(0)

    c_copy.wait()
    latent = held[me]
    row_page = (me * rows + lax.broadcasted_iota(jnp.int32, (1, rows), 1)) // PAGE
    first_page = me * rows // PAGE
    request_of = jnp.zeros((1, rows), jnp.int32)
    for p in range(max(1, rows // PAGE)):
        page = first_page + p
        request = (pt_ref[0, page] * POOL + pt_ref[1, page]) % REQ
        request_of = jnp.where(row_page == page, request, request_of)
    positions = me * cache_dev + lax.broadcasted_iota(jnp.int32, (1, cache_dev), 1)
    nt = (((1,), (1,)), ((), ()))
    for r in range(REQ):
        queries = dq_ref[r]
        keys = ct[r]
        scores = jnp.dot(queries, keys, preferred_element_type=jnp.float32) * SCALE
        page_scores = (
            lax.dot_general(queries, latent, nt, preferred_element_type=jnp.float32) * SCALE
        )
        ok = positions < len_ref[r]
        page_ok = request_of == r
        scores = jnp.where(ok, scores, NEG)
        page_scores = jnp.where(page_ok, page_scores, NEG)
        top = jnp.maximum(
            jnp.max(scores, axis=1, keepdims=True), jnp.max(page_scores, axis=1, keepdims=True)
        )
        weights = jnp.where(ok, jnp.exp(scores - top), 0.0)
        page_weights = jnp.where(page_ok, jnp.exp(page_scores - top), 0.0)
        total = jnp.sum(weights, axis=1, keepdims=True) + jnp.sum(
            page_weights, axis=1, keepdims=True
        )
        mixed = lax.dot_general(
            weights.astype(jnp.bfloat16), keys[:D_LAT], nt, preferred_element_type=jnp.float32
        ) + jnp.dot(
            page_weights.astype(jnp.bfloat16),
            latent[:, :D_LAT],
            preferred_element_type=jnp.float32,
        )
        lane = lax.broadcasted_iota(jnp.int32, (heads, 128), 1)
        tail = jnp.where(lane < 64, top, total)
        parts[:, :, r * MSG : r * MSG + D_LAT] = mixed.reshape(heads, 1, D_LAT)
        parts[:, :, r * MSG + D_LAT : (r + 1) * MSG] = tail.reshape(heads, 1, 128)

    def part_copy(target, source, step):
        return pltpu.make_async_remote_copy(
            src_ref=parts.at[target],
            dst_ref=moved.at[source],
            send_sem=dsend_sem.at[step],
            recv_sem=drecv_sem.at[source],
            device_id={"ctx": target},
        )

    moved[me] = parts[me]

    def send_part(step, carry):
        part_copy((me + step) % n, me, step).start()
        return carry

    lax.fori_loop(1, n, send_part, 0)

    spread_plane(0)
    q_copy.wait()
    for start in range(0, span, 128):
        q[start : start + 128, :] = qt[:, start : start + 128].T
    for step in range(1, line):
        full_wait(block(step, y, x, core))
        spread_column(step)
    for step in range(1, line):
        spread_plane(step)
    for step in range(line):
        half_wait(block(step, far_y, far_x, core))
        to_pair(step, far_y, far_x)
    for step in range(line):
        for by in (y, far_y):
            for bx in (x, far_x):
                full_wait(block(step, by, bx, 1 - core))

    chunk = min(256, span)
    for start in range(0, span, chunk):
        stop = start + chunk
        keys = held[: stop // rows].reshape(stop, held.shape[2])
        scores = lax.dot_general(
            q[start:stop], keys, nt, preferred_element_type=jnp.float32
        )
        row = start + lax.broadcasted_iota(jnp.int32, (chunk, stop), 0)
        col = lax.broadcasted_iota(jnp.int32, (chunk, stop), 1)
        scores = jnp.where(col <= row, scores, NEG)
        top = jnp.max(scores, axis=1, keepdims=True)
        weights = jnp.exp((scores - top) * SCALE)
        total = jnp.sum(weights, axis=1, keepdims=True)
        mixed = jnp.dot(
            weights.astype(jnp.bfloat16), keys[:, :D_LAT], preferred_element_type=jnp.float32
        )
        pout_ref[start:stop, :] = (mixed / total).astype(jnp.bfloat16)

    def await_part(step, carry):
        part_copy((me + step) % n, (me + step) % n, step).wait_recv()
        return carry

    lax.fori_loop(1, n, await_part, 0)
    for r in range(REQ):
        piece = moved[:, :, r * MSG : (r + 1) * MSG].reshape(n, MSG)
        tops = piece[:, D_LAT : D_LAT + 1]
        sums = piece[:, D_LAT + 64 : D_LAT + 65]
        factor = jnp.exp(tops - jnp.max(tops, axis=0, keepdims=True))
        own_sum = jnp.sum(sums * factor, axis=0, keepdims=True)
        own_out = jnp.sum(piece[:, :D_LAT] * factor, axis=0, keepdims=True)
        dout_ref[r : r + 1, :] = (own_out / own_sum).astype(jnp.bfloat16)

    for copy in sends:
        copy.wait_send()

    def drain(step, carry):
        part_copy((me + step) % n, me, step).wait_send()
        return carry

    lax.fori_loop(1, n, drain, 0)


def shards(n, prefill_query, prefill_latent, decode_query, cache, lengths, page_table):
    span, head_here, width = prefill_query.shape
    rows = prefill_latent.shape[0]
    heads = decode_query.shape[1]
    cache_dev = cache.shape[1]
    if head_here != 1 or n % 8 or rows * n != span:
        raise ValueError("unexpected sizes")
    line = n // 8
    vmem = pl.BlockSpec(memory_space=pltpu.VMEM)
    smem = pl.BlockSpec(memory_space=pltpu.SMEM)
    anywhere = pl.BlockSpec(memory_space=pl.ANY)
    dma = pltpu.SemaphoreType.DMA
    prefill_out, decode_out = pl.pallas_call(
        functools.partial(kernel, n),
        out_shape=(
            jax.ShapeDtypeStruct((span, D_LAT), jnp.bfloat16),
            jax.ShapeDtypeStruct((REQ, D_LAT), jnp.bfloat16),
        ),
        in_specs=[anywhere, anywhere, vmem, anywhere, smem, smem],
        out_specs=(vmem, vmem),
        scratch_shapes=[
            pltpu.VMEM((n, rows, width), jnp.bfloat16),
            pltpu.VMEM((width, span), jnp.bfloat16),
            pltpu.VMEM((span, width), jnp.bfloat16),
            pltpu.VMEM((REQ, width, cache_dev), jnp.bfloat16),
            pltpu.VMEM((heads, 1, REQ * MSG), jnp.float32),
            pltpu.VMEM((n, 1, REQ * MSG), jnp.float32),
            dma((3,)),
            dma((line,)),
            dma((line,)),
            dma((line,)),
            dma((line * 4,)),
            dma((line,)),
            dma((line,)),
            dma((n,)),
            dma((n, 2)),
            dma((n,)),
            dma((n,)),
        ],
        compiler_params=pltpu.CompilerParams(collective_id=0, has_side_effects=True),
    )(
        prefill_query[:, 0, :].T,
        prefill_latent,
        decode_query,
        jnp.swapaxes(cache, 1, 2),
        lengths,
        page_table.T,
    )
    return prefill_out[:, None, :], decode_out[:, None, :]


def solution(mesh):
    in_specs = (
        P("groups", "ctx", None),
        P(("groups", "ctx"), None),
        P("groups", None, None),
        P("groups", "ctx", None),
        P("groups"),
        P("groups", None),
    )
    out_specs = (P("groups", "ctx", None), P("groups", "ctx", None))
    return jax.shard_map(
        functools.partial(shards, mesh.shape["ctx"]),
        mesh=mesh,
        in_specs=in_specs,
        out_specs=out_specs,
        check_vma=False,
    )
```

```python
import functools

import jax
import jax.numpy as jnp
from jax import lax
from jax.experimental import pallas as pl
from jax.experimental.pallas import tpu as pltpu
from jax.sharding import PartitionSpec as P

D_LAT = 512
PAGE = 16
POOL = 16
REQ = 2

SCALE = 192.0 ** (-0.5)
NEG = -1e30
MSG = D_LAT + 128


def kernel(
    n,
    qt_hbm,
    lat_hbm,
    dq_hbm,
    ct_hbm,
    len_ref,
    pt_ref,
    pout_ref,
    dout_ref,
    held,
    dq_ref,
    qt,
    q,
    ct,
    parts,
    mate,
    joined,
    moved,
    local_sem,
    z_sem,
    x_sem,
    y_sem,
    pair_sem,
    dx_sem,
    dy_sem,
    full_sem,
    half_sem,
    dsend_sem,
    drecv_sem,
    ready_sem,
    mate_sem,
):
    me = lax.axis_index("ctx")
    line = n // 8
    core = me % 2
    x = (me // 2) % 2
    y = (me // 4) % 2
    z = me // 8
    rows = lat_hbm.shape[0]
    heads = dq_ref.shape[1]
    chips = n // 2
    span = qt.shape[1]
    cache_dev = ct.shape[2]

    def opposite(step):
        result, bit = z, 1
        while bit <= step:
            if step // bit % 2:
                result = result + bit * (1 - 2 * (z // bit % 2))
            bit *= 2
        return result

    lines = [opposite(step) for step in range(line)]

    def block(step, by, bx, bc):
        return ((lines[step] * 2 + by) * 2 + bx) * 2 + bc

    x_peer = block(0, y, 1 - x, core)
    y_peer = block(0, 1 - y, x, core)
    pair = block(0, y, x, 1 - core)

    own_copy = pltpu.make_async_copy(lat_hbm, held.at[me], local_sem.at[0])
    own_copy.start()
    q_copy = pltpu.make_async_copy(qt_hbm, qt, local_sem.at[1])
    q_copy.start()
    c_copy = pltpu.make_async_copy(ct_hbm, ct, local_sem.at[2])
    c_copy.start()
    d_copy = pltpu.make_async_copy(dq_hbm, dq_ref, local_sem.at[3])
    d_copy.start()

    barrier = pltpu.get_barrier_semaphore()

    near = [x_peer, y_peer, pair] + [block(step, y, x, core) for step in range(1, line)]
    for target in near:
        pl.semaphore_signal(barrier, inc=1, device_id={"ctx": target})

    split = rows // 2 if rows % 32 == 0 else rows

    def move(index, send, recv, target, part=None):
        ref = held.at[index]
        if part == 0:
            ref = held.at[index, pl.ds(0, split)]
        if part == 1:
            ref = held.at[index, pl.ds(split, rows - split)]
        return pltpu.make_async_remote_copy(
            src_ref=ref, dst_ref=ref, send_sem=send, recv_sem=recv, device_id={"ctx": target}
        )

    sends = []

    def go(copy):
        copy.start()
        sends.append(copy)

    def to_pair(step, by, bx):
        index = block(step, by, bx, core)
        spot = (step * 2 + (0 if by is y else 1)) * 2 + (0 if bx is x else 1)
        go(move(index, pair_sem.at[spot], full_sem.at[index], pair))

    def full_wait(index):
        move(index, z_sem.at[0], full_sem.at[index], pair).wait_recv()

    def half_wait(index):
        move(index, z_sem.at[0], half_sem.at[index, 0], pair, 0).wait_recv()
        if split < rows:
            move(index, z_sem.at[0], half_sem.at[index, 1], pair, 1).wait_recv()

    far_x, far_y = 1 - x, 1 - y

    def spread_column(step):
        index = block(step, y, x, core)
        go(move(index, x_sem.at[step], full_sem.at[index], x_peer))
        go(move(index, y_sem.at[step], full_sem.at[index], y_peer))
        to_pair(step, y, x)

    def spread_plane(step):
        index = block(step, y, far_x, core)
        full_wait(index)
        if split < rows:
            go(move(index, dy_sem.at[step], half_sem.at[index, 1], y_peer, 1))
        to_pair(step, y, far_x)
        index = block(step, far_y, x, core)
        full_wait(index)
        go(move(index, dx_sem.at[step], half_sem.at[index, 0], x_peer, 0))
        to_pair(step, far_y, x)

    q_copy.wait()
    for start in range(0, span, 128):
        q[start : start + 128, :] = qt[:, start : start + 128].T
    own_copy.wait()
    pl.semaphore_wait(barrier, len(near))

    pl.semaphore_signal(ready_sem.at[0], inc=1, device_id={"ctx": x_peer})
    spread_column(0)
    for step in range(1, line):
        go(move(me, z_sem.at[step], full_sem.at[me], block(step, y, x, core)))
    c_copy.wait()
    d_copy.wait()
    latent = held[me]
    row_page = (me * rows + lax.broadcasted_iota(jnp.int32, (1, rows), 1)) // PAGE
    first_page = me * rows // PAGE
    request_of = jnp.zeros((1, rows), jnp.int32)
    for p in range(max(1, rows // PAGE)):
        page = first_page + p
        request = (pt_ref[0, page] * POOL + pt_ref[1, page]) % REQ
        request_of = jnp.where(row_page == page, request, request_of)
    positions = me * cache_dev + lax.broadcasted_iota(jnp.int32, (1, cache_dev), 1)
    nt = (((1,), (1,)), ((), ()))
    for r in range(REQ):
        queries = dq_ref[r]
        keys = ct[r]
        scores = jnp.dot(queries, keys, preferred_element_type=jnp.float32) * SCALE
        page_scores = (
            lax.dot_general(queries, latent, nt, preferred_element_type=jnp.float32) * SCALE
        )
        ok = positions < len_ref[r]
        page_ok = request_of == r
        scores = jnp.where(ok, scores, NEG)
        page_scores = jnp.where(page_ok, page_scores, NEG)
        top = jnp.maximum(
            jnp.max(scores, axis=1, keepdims=True), jnp.max(page_scores, axis=1, keepdims=True)
        )
        weights = jnp.where(ok, jnp.exp(scores - top), 0.0)
        page_weights = jnp.where(page_ok, jnp.exp(page_scores - top), 0.0)
        total = jnp.sum(weights, axis=1, keepdims=True) + jnp.sum(
            page_weights, axis=1, keepdims=True
        )
        mixed = lax.dot_general(
            weights.astype(jnp.bfloat16), keys[:D_LAT], nt, preferred_element_type=jnp.float32
        ) + jnp.dot(
            page_weights.astype(jnp.bfloat16),
            latent[:, :D_LAT],
            preferred_element_type=jnp.float32,
        )
        lane = lax.broadcasted_iota(jnp.int32, (heads, 128), 1)
        tail = jnp.where(lane < 64, top, total)
        parts[:, :, :, r * MSG : r * MSG + D_LAT] = mixed.reshape(chips, 2, 1, D_LAT)
        parts[:, :, :, r * MSG + D_LAT : (r + 1) * MSG] = tail.reshape(chips, 2, 1, 128)

    mate_copy = pltpu.make_async_remote_copy(
        src_ref=parts.at[:, 1 - core],
        dst_ref=mate,
        send_sem=mate_sem.at[0],
        recv_sem=mate_sem.at[1],
        device_id={"ctx": pair},
    )
    mate_copy.start()

    def part_copy(target, source):
        return pltpu.make_async_remote_copy(
            src_ref=joined.at[target],
            dst_ref=moved.at[source],
            send_sem=dsend_sem.at[target],
            recv_sem=drecv_sem.at[source],
            device_id={"ctx": target * 2 + core},
        )

    chip = me // 2

    def ready(stage, target):
        pl.semaphore_signal(ready_sem.at[stage], inc=1, device_id={"ctx": target})

    def send_part(step, carry):
        part_copy((chip + step) % chips, chip).start()
        return carry

    def join():
        mate_copy.wait_recv()
        for r in range(REQ):
            mine = parts[:, core, :, r * MSG : (r + 1) * MSG].reshape(chips, MSG)
            other = mate[:, :, r * MSG : (r + 1) * MSG].reshape(chips, MSG)
            top_mine = mine[:, D_LAT : D_LAT + 1]
            top_other = other[:, D_LAT : D_LAT + 1]
            top = jnp.maximum(top_mine, top_other)
            both = mine * jnp.exp(top_mine - top) + other * jnp.exp(top_other - top)
            lane = lax.broadcasted_iota(jnp.int32, (chips, 128), 1)
            tail = jnp.where(lane < 64, top, both[:, D_LAT:])
            joined[:, :, r * MSG : r * MSG + D_LAT] = both[:, :D_LAT].reshape(chips, 1, D_LAT)
            joined[:, :, r * MSG + D_LAT : (r + 1) * MSG] = tail.reshape(chips, 1, 128)
        moved[chip] = joined[chip]

    pl.semaphore_wait(ready_sem.at[0], 1)
    ready(1, y_peer)
    spread_plane(0)
    join()
    pl.semaphore_wait(ready_sem.at[1], 1)
    lax.fori_loop(1, chips, send_part, 0)
    for step in range(1, line):
        full_wait(block(step, y, x, core))
        spread_column(step)
    for step in range(1, line):
        spread_plane(step)
    for step in range(line):
        index = block(step, far_y, far_x, core)
        half_wait(index)
        to_pair(step, far_y, far_x)
    for step in range(line):
        for by in (y, far_y):
            for bx in (x, far_x):
                index = block(step, by, bx, 1 - core)
                full_wait(index)

    chunk = min(256, span)
    for start in range(0, span, chunk):
        stop = start + chunk
        keys = held[: stop // rows].reshape(stop, held.shape[2])
        scores = lax.dot_general(
            q[start:stop], keys, nt, preferred_element_type=jnp.float32
        )
        row = start + lax.broadcasted_iota(jnp.int32, (chunk, stop), 0)
        col = lax.broadcasted_iota(jnp.int32, (chunk, stop), 1)
        scores = jnp.where(col <= row, scores, NEG)
        top = jnp.max(scores, axis=1, keepdims=True)
        weights = jnp.exp((scores - top) * SCALE)
        total = jnp.sum(weights, axis=1, keepdims=True)
        mixed = jnp.dot(
            weights.astype(jnp.bfloat16), keys[:, :D_LAT], preferred_element_type=jnp.float32
        )
        pout_ref[start:stop, :] = (mixed / total).astype(jnp.bfloat16)

    def await_part(step, carry):
        source = (chip + step) % chips
        part_copy(source, source).wait_recv()
        return carry

    lax.fori_loop(1, chips, await_part, 0)
    for r in range(REQ):
        piece = moved[:, :, r * MSG : (r + 1) * MSG].reshape(chips, MSG)
        tops = piece[:, D_LAT : D_LAT + 1]
        sums = piece[:, D_LAT + 64 : D_LAT + 65]
        factor = jnp.exp(tops - jnp.max(tops, axis=0, keepdims=True))
        own_sum = jnp.sum(sums * factor, axis=0, keepdims=True)
        own_out = jnp.sum(piece[:, :D_LAT] * factor, axis=0, keepdims=True)
        dout_ref[r : r + 1, :] = (own_out / own_sum).astype(jnp.bfloat16)

    for copy in sends:
        copy.wait_send()

    def drain(step, carry):
        part_copy((chip + step) % chips, chip).wait_send()
        return carry

    mate_copy.wait_send()
    lax.fori_loop(1, chips, drain, 0)


def shards(n, prefill_query, prefill_latent, decode_query, cache, lengths, page_table):
    span, head_here, width = prefill_query.shape
    rows = prefill_latent.shape[0]
    heads = decode_query.shape[1]
    cache_dev = cache.shape[1]
    if head_here != 1 or n % 8 or rows * n != span:
        raise ValueError("unexpected sizes")
    line = n // 8
    vmem = pl.BlockSpec(memory_space=pltpu.VMEM)
    smem = pl.BlockSpec(memory_space=pltpu.SMEM)
    anywhere = pl.BlockSpec(memory_space=pl.ANY)
    dma = pltpu.SemaphoreType.DMA
    prefill_out, decode_out = pl.pallas_call(
        functools.partial(kernel, n),
        out_shape=(
            pltpu.VMEM((span, D_LAT), jnp.bfloat16),
            pltpu.VMEM((REQ, D_LAT), jnp.bfloat16),
        ),
        in_specs=[anywhere, anywhere, anywhere, anywhere, smem, smem],
        out_specs=(vmem, vmem),
        scratch_shapes=[
            pltpu.VMEM((n, rows, width), jnp.bfloat16),
            pltpu.VMEM((REQ, heads, width), jnp.bfloat16),
            pltpu.VMEM((width, span), jnp.bfloat16),
            pltpu.VMEM((span, width), jnp.bfloat16),
            pltpu.VMEM((REQ, width, cache_dev), jnp.bfloat16),
            pltpu.VMEM((n // 2, 2, 1, REQ * MSG), jnp.float32),
            pltpu.VMEM((n // 2, 1, REQ * MSG), jnp.float32),
            pltpu.VMEM((n // 2, 1, REQ * MSG), jnp.float32),
            pltpu.VMEM((n // 2, 1, REQ * MSG), jnp.float32),

            dma((4,)),
            dma((line,)),
            dma((line,)),
            dma((line,)),
            dma((line * 4,)),
            dma((line,)),
            dma((line,)),
            dma((n,)),
            dma((n, 2)),
            dma((n // 2,)),
            dma((n // 2,)),
            pltpu.SemaphoreType.REGULAR((2,)),
            dma((2,)),
        ],
        compiler_params=pltpu.CompilerParams(collective_id=0, has_side_effects=True),
    )(
        prefill_query[:, 0, :].T,
        prefill_latent,
        decode_query,
        jnp.swapaxes(cache, 1, 2),
        lengths,
        page_table.T,
    )
    return prefill_out[:, None, :], decode_out[:, None, :]


def solution(mesh):
    in_specs = (
        P("groups", "ctx", None),
        P(("groups", "ctx"), None),
        P("groups", None, None),
        P("groups", "ctx", None),
        P("groups"),
        P("groups", None),
    )
    out_specs = (P("groups", "ctx", None), P("groups", "ctx", None))
    return jax.shard_map(
        functools.partial(shards, mesh.shape["ctx"]),
        mesh=mesh,
        in_specs=in_specs,
        out_specs=out_specs,
        check_vma=False,
    )
```
